32 devices in a mesh: groups: 2 (over x), seq: 8 (over z, y), mp: 2 (over core).
Axes of the slice: x: 2, y: 2, z: 4, core: 2. Of those that a mesh axis runs over, the one named last changes fastest.
Arguments:
- latent_cache: bfloat16 [2048, 64, 512], P(('groups', 'seq')), parts along dimension 0, may hold values from -6 to 6
- rope_cache: bfloat16 [2048, 4096], P(('groups', 'seq')), parts along dimension 0, may hold values from -6 to 6
- q_nope: bfloat16 [16, 128, 128], P('groups', 'mp'), parts along dimension 0, may hold values from -12 to 12
- q_rope: bfloat16 [16, 128, 64], P('groups', 'mp'), parts along dimension 0, may hold values from -2000 to 2000
- w_uk: bfloat16 [128, 128, 512], P('mp', None, 'seq'), may hold values from -0.5 to 0.5
- value_up_weight: bfloat16 [128, 512, 128], P('mp', 'seq'), may hold values from -0.25 to 0.25
- w_out: bfloat16 [16384, 7168], P('mp', 'seq'), may hold values from -0.046875 to 0.046875
- page_table: int32 [16, 256], P('groups'), parts along dimension 0, may hold values from 0 to 1023, as said below
- lengths: int32 [16], P('groups'), parts along dimension 0, may hold values from 2048 to 16384, as said below
Outputs:
- output: bfloat16 [16, 7168], P('groups', ('seq', 'mp')), parts along dimension 0
The draws below stay inside these ranges and needn't reach their ends.
There are 2 independent parts, one for each index of `groups`. The reference program is written for one: setup_inputs(seed, part) draws one part's arguments, and reference() takes and returns one part's arrays. A program takes and returns all parts, laid end to end along the dimension named above; an argument that names none is the same for every part. Nothing has to cross between parts.
Inputs may be any that keep to these rules, and one draw needn't show every extreme that they name: `lengths`: every sequence has one eighth of 16384 tokens or more; the longest has exactly 16384. page_table[b,p] for p < ceil(lengths[b] / 64) is the global slot (shard index times 128 plus local slot) holding that page; these live entries are all distinct; the other entries are 0 and unused.
All inputs are finite; a program needn't handle non-finite values.
Results may differ from the reference program's by a relative error of at most 0.012.
Values may be sent and summed in bfloat16 or wider, within the bound.
A program may use at most 128 MiB of HBM per device.

```python
import jax
import jax.numpy as jnp
from jax import lax

B = 8
H = 128
NOPE = 128
ROPE = 64
KVR = 512
VDIM = 128
D = 7168
PAGE = 64
SLOTS_DEV = 128
SLOTS = 1024
MAXLEN = 16384
MAXPAGES = 256
N_SEQ = 8


def page_layout(key):
    key_len, key_long, key_weight, key_perm = jax.random.split(jax.random.fold_in(key, 11), 4)
    others = jax.random.randint(key_len, (B,), MAXLEN // 8, MAXLEN // 4 + 1)
    longest_length = jax.random.randint(key_long, (), 0, B)
    lengths = jnp.where(jnp.arange(B) == longest_length, MAXLEN, others).astype(jnp.int32)
    page_count = (lengths + PAGE - 1) // PAGE
    offsets = jnp.cumsum(page_count) - page_count
    weight = jax.random.randint(key_weight, (N_SEQ,), 0, 4)
    shuffled = jax.random.permutation(key_perm, SLOTS)
    ranking = jnp.repeat(weight, SLOTS_DEV) * SLOTS + shuffled
    slot_order = jnp.argsort(-ranking)
    logical = jnp.arange(MAXPAGES)
    position = jnp.clip(offsets[:, None] + logical[None, :], 0, SLOTS - 1)
    page_map = jnp.where(logical[None, :] < page_count[:, None], slot_order[position], 0).astype(jnp.int32)
    return (lengths, page_map)


def rope_values(key):
    base = jnp.clip(jax.random.normal(jax.random.fold_in(key, 23), (SLOTS, PAGE, ROPE), jnp.float32), -6.0, 6.0)
    return base


def draw_lengths(key, part):
    return page_layout(key)[0]


def draw_page_table(key, part):
    return page_layout(key)[1]


def draw_rope_cache(key, part):
    return rope_values(key).reshape(SLOTS, PAGE * ROPE).astype(jnp.bfloat16)


def draw_q_rope(key, part):
    drawn = jnp.clip(2.0 * jax.random.normal(jax.random.fold_in(key, 31), (B, H, ROPE), jnp.float32), -12.0, 12.0)
    return drawn.astype(jnp.bfloat16)


def steps_of(key, dims, shards, low, high):
    gain, own = 1.0, jax.random.fold_in(key, 6)
    for dim, blocks in shards:
        steps = jnp.exp(jax.random.uniform(jax.random.fold_in(own, dim), (blocks,), jnp.float32, low / len(shards), high / len(shards)))
        gain = gain * jnp.repeat(steps, dims[dim] // blocks).reshape([-1 if axis == dim else 1 for axis in range(len(dims))])
    return gain


def gaussian(rng, extent, deviation, limit, cuts=(), held_as=jnp.bfloat16):
    gain = steps_of(rng, extent, cuts, -0.22, 0.18) if cuts else 1.0
    values = jax.random.normal(rng, extent, jnp.float32) * deviation * gain
    return jnp.minimum(jnp.maximum(values, -limit), limit).astype(held_as)


def setup_inputs(seed: int = 0, part: int = 0) -> dict:
    splits = jax.random.split(jax.random.key(seed), 10)
    part_keys = jax.random.split(jax.random.fold_in(splits[9], part), 10)
    latent_cache = gaussian(part_keys[0], (SLOTS, PAGE, KVR), 1.0, 6.0, ((0, 8),))
    rope_cache = draw_rope_cache(jax.random.fold_in(jax.random.fold_in(splits[9], part), 71), part)
    q_nope = gaussian(part_keys[2], (B, H, NOPE), 2.0, 12.0, ((1, 2),))
    q_rope = draw_q_rope(jax.random.fold_in(jax.random.fold_in(splits[9], part), 71), part)
    w_uk = gaussian(splits[4], (H, NOPE, KVR), NOPE ** -0.5, 0.5, ((0, 2), (2, 8)))
    value_up_weight = gaussian(splits[5], (H, KVR, VDIM), KVR ** -0.5, 0.25, ((0, 2), (1, 8)))
    w_out = gaussian(splits[6], (H * VDIM, D), (H * VDIM) ** -0.5, 0.046875, ((0, 2), (1, 8)))
    page_table = draw_page_table(jax.random.fold_in(jax.random.fold_in(splits[9], part), 71), part)
    lengths = draw_lengths(jax.random.fold_in(jax.random.fold_in(splits[9], part), 71), part)
    return dict(latent_cache=latent_cache, rope_cache=rope_cache, q_nope=q_nope, q_rope=q_rope, w_uk=w_uk, value_up_weight=value_up_weight, w_out=w_out, page_table=page_table, lengths=lengths)


NEG = -1.0e30


def reference(latent_cache, rope_cache, q_nope, q_rope, w_uk, value_up_weight, w_out, page_table, lengths):
    score_scale = (NOPE + ROPE) ** -0.5
    peak_score = lax.Precision.HIGHEST
    q_latent = jnp.einsum('bhn,hnk->bhk', q_nope.astype(jnp.float32), w_uk.astype(jnp.float32), precision=peak_score).astype(jnp.bfloat16)
    page_count = (lengths + PAGE - 1) // PAGE
    logical = jnp.arange(MAXPAGES, dtype=jnp.int32)
    live_page = logical[None, :] < page_count[:, None]
    tokens_in = jnp.clip(lengths[:, None] - PAGE * logical[None, :], 0, PAGE).astype(jnp.int32)
    target = jnp.where(live_page, page_table, SLOTS).astype(jnp.int32).reshape(-1)
    seq_ids = jnp.broadcast_to(jnp.arange(B, dtype=jnp.int32)[:, None], (B, MAXPAGES)).reshape(-1)
    slot_owner = jnp.zeros((SLOTS, B), jnp.float32).at[target, seq_ids].set(1.0, mode='drop')
    slot_fill = jnp.zeros((SLOTS,), jnp.int32).at[target].add(tokens_in.reshape(-1), mode='drop')
    blocks = SLOTS // 8
    latent_blocks = latent_cache.reshape(blocks, 8, PAGE, KVR)
    rope_blocks = rope_cache.reshape(blocks, 8, PAGE, ROPE)
    owner_blocks = slot_owner.reshape(blocks, 8, B)
    fill_blocks = slot_fill.reshape(blocks, 8)
    q_latent_f = q_latent.astype(jnp.float32)
    q_rope_f = q_rope.astype(jnp.float32)

    def step_block(run_state, block_data):
        run_max, run_sum, run_out = run_state
        latent_block, rope_block, owner_block, fill_block = block_data
        latent_f = latent_block.astype(jnp.float32)
        pick_latent = jnp.einsum('sb,bhk->shk', owner_block, q_latent_f, precision=peak_score)
        pick_rope = jnp.einsum('sb,bhr->shr', owner_block, q_rope_f, precision=peak_score)
        scores = (jnp.einsum('shk,stk->sht', pick_latent, latent_f, precision=peak_score)
                  + jnp.einsum('shr,str->sht', pick_rope, rope_block.astype(jnp.float32), precision=peak_score)) * score_scale
        live_token = jnp.arange(PAGE, dtype=jnp.int32)[None, None, :] < fill_block[:, None, None]
        slot_max = jnp.max(jnp.where(live_token, scores, NEG), axis=2)
        exponent = jnp.where(live_token, jnp.exp(scores - slot_max[:, :, None]), 0.0)
        slot_sum = jnp.sum(exponent, axis=2)
        weights = lax.optimization_barrier(exponent.astype(jnp.bfloat16)).astype(jnp.float32)
        slot_out = jnp.einsum('sht,stk->shk', weights, latent_f, precision=peak_score)
        owned = jnp.transpose(owner_block) > 0
        candidate = jnp.where(owned[:, :, None], slot_max[None, :, :], NEG)
        new_max = jnp.maximum(run_max, jnp.max(candidate, axis=1))
        carry_scale = jnp.exp(run_max - new_max)
        factor = jnp.where(owned[:, :, None], jnp.exp(candidate - new_max[:, None, :]), 0.0)
        run_sum = run_sum * carry_scale + jnp.einsum('bsh,sh->bh', factor, slot_sum, precision=peak_score)
        run_out = run_out * carry_scale[:, :, None] + jnp.einsum('bsh,shk->bhk', factor, slot_out, precision=peak_score)
        return (new_max, run_sum, run_out), None

    initial = (jnp.full((B, H), NEG, jnp.float32), jnp.zeros((B, H), jnp.float32), jnp.zeros((B, H, KVR), jnp.float32))
    final_state, unused = lax.scan(step_block, initial, (latent_blocks, rope_blocks, owner_blocks, fill_blocks))
    seq_max, seq_sum, seq_out = final_state
    attention_probs = (seq_out / seq_sum[:, :, None]).astype(jnp.bfloat16)
    value_rows = jnp.einsum('gre,req->grq', attention_probs.astype(jnp.float32), value_up_weight.astype(jnp.float32), precision=peak_score).astype(jnp.bfloat16)
    output = jnp.dot(value_rows.reshape(B, H * VDIM), w_out, preferred_element_type=jnp.float32).astype(jnp.bfloat16)
    return output
```

```python
import functools

import jax
import jax.numpy as jnp
from jax import lax
from jax.experimental import pallas as pl
from jax.experimental.pallas import tpu as pltpu
from jax.sharding import PartitionSpec as P

NEG = -1e30
MESH = pl.DeviceIdType.MESH
GROUP = 8
F32 = jnp.float32
BF16 = jnp.bfloat16


def greet(n, me, partner=None):
    barrier = pltpu.get_barrier_semaphore()
    for k in range(1, n):
        peer = lax.rem(me + k, n)
        pl.semaphore_signal(barrier, inc=1, device_id={"seq": peer}, device_id_type=MESH)
    if partner is not None:
        pl.semaphore_signal(barrier, inc=1, device_id={"mp": partner}, device_id_type=MESH)
    pl.semaphore_wait(barrier, n - 1 + (partner is not None))


def push(n, me, src_of, dst, send, recv):
    copies = []
    for k in range(1, n):
        peer = lax.rem(me + k, n)
        copy = pltpu.make_async_remote_copy(
            src_ref=src_of(peer), dst_ref=dst.at[me], send_sem=send.at[k], recv_sem=recv.at[k],
            device_id={"seq": peer}, device_id_type=MESH,
        )
        copy.start()
        copies.append(copy)
    return copies


def query_kernel(n, pack, q_ref, w_ref, out_ref, raw, gath, send, recv):
    me = lax.axis_index("seq")
    heads, seqs, _ = q_ref.shape
    cols = w_ref.shape[2]
    greet(n, me)
    for h in range(heads):
        raw[h * seqs:(h + 1) * seqs, :] = jnp.dot(q_ref[h], w_ref[h], preferred_element_type=F32)
    for b in range(0, seqs, pack):
        parts = [raw[pl.ds(b + j, heads, stride=seqs), :] for j in range(pack)]
        row = parts[0] if pack == 1 else jnp.concatenate(parts, axis=1)
        gath[me, b // pack * heads:(b // pack + 1) * heads, :] = row.astype(BF16)
    copies = push(n, me, lambda peer: gath.at[me], gath, send, recv)
    for copy in copies:
        copy.wait()
    for s in range(n):
        for b in range(seqs):
            lane = b % pack * cols
            out_ref[b, :, s * cols:(s + 1) * cols] = gath[
                s, b // pack * heads:(b // pack + 1) * heads, lane:lane + cols]


def attend_kernel(scale, pack, slots_ref, fills_ref, owner_ref, count_ref, q_ref, qr_ref, rope_ref, latent_ref,
                  out_ref, kbuf, acc, top, total, sems):
    seqs, heads, width = q_ref.shape
    page = latent_ref.shape[1]
    half = rope_ref.shape[1]
    tokens = GROUP * page
    n = out_ref.shape[0]
    cols = width // n
    count = count_ref[0]
    acc[...] = jnp.zeros_like(acc)
    top[...] = jnp.full(top.shape, NEG, F32)
    total[...] = jnp.zeros_like(total)

    def fetch(c, buf):
        return [pltpu.make_async_copy(
            latent_ref.at[slots_ref[c * GROUP + g]], kbuf.at[buf, pl.ds(g * page, page)], sems.at[buf, g])
            for g in range(GROUP)]

    for ahead in range(2):
        @pl.when(count > ahead)
        def _():
            for copy in fetch(ahead, ahead):
                copy.start()

    lane = lax.broadcasted_iota(jnp.int32, (1, tokens), 1)
    rows2 = GROUP * half
    spread = (lax.broadcasted_iota(jnp.int32, (tokens, rows2), 0) // (page // half)
              == lax.broadcasted_iota(jnp.int32, (tokens, rows2), 1)).astype(F32).astype(BF16)
    per = page // half
    rope_w = 128 // per
    keep = (lax.broadcasted_iota(jnp.int32, (tokens, 128), 0) % per
            == lax.broadcasted_iota(jnp.int32, (tokens, 128), 1) // rope_w)

    def step(c, _):
        buf = lax.rem(c, 3)

        @pl.when(c + 2 < count)
        def _():
            for copy in fetch(c + 2, lax.rem(c + 2, 3)):
                copy.start()

        b = owner_ref[c]
        rope = jnp.concatenate([rope_ref[slots_ref[c * GROUP + g]] for g in range(GROUP)], axis=0)
        rope = jnp.dot(spread, rope, preferred_element_type=F32)
        rope = jnp.where(keep, rope, 0.0).astype(BF16)
        limit = jnp.zeros((1, tokens), jnp.int32)
        for g in range(GROUP):
            limit = jnp.where(lane // page == g, fills_ref[c * GROUP + g] + g * page, limit)
        nt = (((1,), (1,)), ((), ()))
        score = lax.dot_general(qr_ref[b], rope, nt, preferred_element_type=F32)
        for copy in fetch(c, buf):
            copy.wait()
        keys = kbuf[buf]
        score = (score + lax.dot_general(q_ref[b], keys, nt, preferred_element_type=F32)) * scale
        score = jnp.where(lane < limit, score, NEG)
        old = top[b][:, :1]
        new = jnp.maximum(old, jnp.max(score, axis=1, keepdims=True))
        weight = jnp.exp(score - new)
        carry = jnp.exp(old - new)
        total[b] = total[b] * carry + jnp.sum(weight, axis=1, keepdims=True)
        top[b] = jnp.broadcast_to(new, top.shape[1:])
        acc[b] = acc[b] * carry + jnp.dot(weight.astype(BF16), keys, preferred_element_type=F32)
        return 0

    lax.fori_loop(0, count, step, 0)

    ids = lax.broadcasted_iota(jnp.int32, (heads, 128), 1)
    extra = jnp.zeros((heads, 128), F32)
    for b in range(seqs):
        inv = 1.0 / jnp.maximum(total[b][:, :1], 1e-30)
        whole = acc[b] * inv
        for s in range(n):
            at = b % pack * cols
            out_ref[s, b // pack * heads:(b // pack + 1) * heads, at:at + cols] = whole[
                :, s * cols:(s + 1) * cols].astype(BF16)
        for k, value in enumerate((top[b], total[b])):
            for j in range(3):
                term = value.astype(BF16).astype(F32)
                extra = jnp.where(ids == b * 6 + k * 3 + j, term, extra)
                value = value - term
    base = seqs // pack * heads
    lanes = out_ref.shape[2]
    for s in range(n):
        out_ref[s, base:base + heads, :] = extra[:, :lanes].astype(BF16)


def finish_kernel(n, pack, o_ref, v_ref, w_hbm, out_ref, gath, port, pv, part, vals, lhs, w_buf, res,
                  tx, rx, send1, recv1, send2, recv2, send3, recv3, send4, recv4, wsem):
    me = lax.axis_index("seq")
    half = lax.axis_index("mp")
    heads, cols, vdim = v_ref.shape
    seqs = lhs.shape[0]
    hs = heads // n
    load = pltpu.make_async_copy(w_hbm, w_buf, wsem)
    load.start()
    greet(n, me, 1 - half)
    copies = push(n, me, lambda peer: o_ref.at[peer], gath, send1, recv1)
    gath[me] = o_ref[me]
    for copy in copies:
        copy.wait()

    base = seqs // pack * heads
    for p in range(seqs // pack):
        mixed = [None] * pack
        for j in range(pack):
            b = p * pack + j
            tops, sums = [], []
            for s in range(n):
                e = gath[s, base:base + heads, :].astype(F32)
                tops.append(e[:, 6 * b:6 * b + 1] + e[:, 6 * b + 1:6 * b + 2] + e[:, 6 * b + 2:6 * b + 3])
                sums.append(e[:, 6 * b + 3:6 * b + 4] + e[:, 6 * b + 4:6 * b + 5] + e[:, 6 * b + 5:6 * b + 6])
            best = functools.reduce(jnp.maximum, tops)
            scaled = [x * jnp.exp(t - best) for t, x in zip(tops, sums)]
            inv = 1.0 / functools.reduce(jnp.add, scaled)
            total = 0.0
            for s in range(n):
                piece = gath[s, p * heads:(p + 1) * heads, j * cols:(j + 1) * cols].astype(F32)
                total = total + piece * (scaled[s] * inv)
            port[b * heads:(b + 1) * heads, :] = total
    for h in range(heads):
        x = port[pl.ds(h, seqs, stride=heads), :].astype(BF16)
        pv[h // hs, h % hs * seqs:(h % hs + 1) * seqs, :] = jnp.dot(
            x, v_ref[h], preferred_element_type=F32).astype(BF16)
    copies = push(n, me, lambda peer: pv.at[peer], part, send2, recv2)
    part[me] = pv[me]
    for copy in copies:
        copy.wait()
    total = part[0].astype(F32)
    for s in range(1, n):
        total = total + part[s].astype(F32)
    vals[me] = total.astype(BF16)
    copies = push(n, me, lambda peer: vals.at[me], vals, send3, recv3)
    for copy in copies:
        copy.wait()
    for h in range(heads):
        lhs[:, h * vdim:(h + 1) * vdim] = vals[h // hs, h % hs * seqs:(h % hs + 1) * seqs, :]
    load.wait()
    rows = w_buf.shape[0]
    res[...] = jnp.zeros_like(res)
    cut = 1024

    def body(i, _):
        at = pl.ds(pl.multiple_of(i * cut, cut), cut)
        res[...] += jnp.dot(lhs[:, at], w_buf[at, :], preferred_element_type=F32)
        return 0

    lax.fori_loop(0, rows // cut, body, 0)
    wide = res.shape[1] // 2
    low, high = res[:, :wide], res[:, wide:]
    first = half == 0
    tx[...] = jnp.where(first, high, low)
    copy = pltpu.make_async_remote_copy(
        src_ref=tx, dst_ref=rx, send_sem=send4, recv_sem=recv4,
        device_id={"mp": 1 - half}, device_id_type=MESH)
    copy.start()
    copy.wait()
    out_ref[...] = (jnp.where(first, low, high) + rx[...]).astype(BF16)


def plan(page_table, lengths, slots_dev, page):
    seqs, pages = page_table.shape
    first_slot = lax.axis_index("seq") * slots_dev
    page_count = (lengths + page - 1) // page
    logical = jnp.arange(pages, dtype=jnp.int32)
    live = logical[None, :] < page_count[:, None]
    tokens_in = jnp.clip(lengths[:, None] - page * logical[None, :], 0, page)
    ids = jnp.arange(slots_dev, dtype=jnp.int32)
    hits = ((page_table - first_slot)[:, :, None] == ids[None, None, :]) & live[:, :, None]
    fill = jnp.sum(jnp.where(hits, tokens_in[:, :, None], 0), axis=1)
    owned = (fill > 0).astype(jnp.int32)
    steps = (jnp.sum(owned, axis=1) + GROUP - 1) // GROUP
    before = jnp.arange(seqs)[:, None] > jnp.arange(seqs)[None, :]
    start = jnp.sum(jnp.where(before, steps[None, :], 0), axis=1)
    earlier = (ids[:, None] < ids[None, :]).astype(F32)
    place = jnp.dot(owned.astype(F32), earlier, precision=lax.Precision.HIGHEST).astype(jnp.int32)
    target = jnp.sum(jnp.where(owned > 0, start[:, None] * GROUP + place + 1, 0), axis=0) - 1
    most = (slots_dev + seqs * (GROUP - 1)) // GROUP
    at = jnp.arange(most * GROUP, dtype=jnp.int32)
    match = at[:, None] == target[None, :]
    slots = jnp.sum(jnp.where(match, ids[None, :], 0), axis=1)
    fills = jnp.sum(jnp.where(match, jnp.sum(fill, axis=0)[None, :], 0), axis=1)
    ends = start + steps
    owner = jnp.sum((jnp.arange(most)[:, None] >= ends[None, :]).astype(jnp.int32), axis=1)
    owner = jnp.minimum(owner, seqs - 1)
    return slots, fills, owner, jnp.sum(steps).reshape(1)


def local(n, latent_cache, rope_cache, q_nope, q_rope, w_uk, value_up_weight, w_out, page_table, lengths):
    slots_dev, page, width = latent_cache.shape
    seqs, heads, nope = q_nope.shape
    rope_w = q_rope.shape[2]
    cols = w_uk.shape[2]
    vdim = value_up_weight.shape[2]
    scale = (nope + rope_w) ** (-0.5)
    pack = max(1, min(seqs, 128 // cols))
    lanes = pack * cols
    vm = pl.BlockSpec(memory_space=pltpu.VMEM)
    sm = pl.BlockSpec(memory_space=pltpu.SMEM)
    hbm = pl.BlockSpec(memory_space=pl.ANY)
    dma = pltpu.SemaphoreType.DMA
    params = functools.partial(pltpu.CompilerParams, has_side_effects=True)

    q_latent = pl.pallas_call(
        functools.partial(query_kernel, n, pack),
        out_shape=jax.ShapeDtypeStruct((seqs, heads, width), BF16),
        in_specs=[vm, vm], out_specs=vm,
        scratch_shapes=[
            pltpu.VMEM((heads * seqs, cols), F32),
            pltpu.VMEM((n, seqs // pack * heads, lanes), BF16),
            dma((n,)), dma((n,)),
        ],
        compiler_params=params(collective_id=1), name="queries",
    )(q_nope.transpose(1, 0, 2), w_uk)

    slots, fills, owner, count = plan(page_table, lengths, slots_dev, page)
    per = 128 // rope_w
    rope = rope_cache.reshape(slots_dev, page // per, 128)
    rows = seqs // pack * heads + heads
    mixed = pl.pallas_call(
        functools.partial(attend_kernel, scale, pack),
        out_shape=jax.ShapeDtypeStruct((n, rows, lanes), BF16),
        in_specs=[sm, sm, sm, sm, vm, vm, vm, hbm], out_specs=vm,
        scratch_shapes=[
            pltpu.VMEM((3, GROUP * page, width), BF16),
            pltpu.VMEM((seqs, heads, width), F32),
            pltpu.VMEM((seqs, heads, 128), F32),
            pltpu.VMEM((seqs, heads, 128), F32),
            dma((3, GROUP)),
        ],
        name="attend",
    )(slots, fills, owner, count, q_latent, jnp.concatenate([q_rope] * per, axis=2), rope, latent_cache)

    wide = w_out.shape[1]
    hs = heads // n
    return pl.pallas_call(
        functools.partial(finish_kernel, n, pack),
        out_shape=jax.ShapeDtypeStruct((seqs, wide // 2), BF16),
        in_specs=[vm, vm, hbm], out_specs=vm,
        scratch_shapes=[
            pltpu.VMEM((n, rows, lanes), BF16),
            pltpu.VMEM((seqs * heads, cols), F32),
            pltpu.VMEM((n, hs * seqs, vdim), BF16),
            pltpu.VMEM((n, hs * seqs, vdim), BF16),
            pltpu.VMEM((n, hs * seqs, vdim), BF16),
            pltpu.VMEM((seqs, heads * vdim), BF16),
            pltpu.VMEM(w_out.shape, BF16),
            pltpu.VMEM((seqs, wide), F32),
            pltpu.VMEM((seqs, wide // 2), F32),
            pltpu.VMEM((seqs, wide // 2), F32),
            dma((n,)), dma((n,)), dma((n,)), dma((n,)), dma((n,)), dma((n,)), dma, dma, dma,
        ],
        compiler_params=params(collective_id=2, vmem_limit_bytes=48 * 1024 * 1024), name="finish",
    )(mixed, value_up_weight, w_out)


def solution(mesh):
    return jax.shard_map(
        functools.partial(local, mesh.shape["seq"]),
        mesh=mesh,
        in_specs=(
            P(("groups", "seq"), None, None),
            P(("groups", "seq"), None),
            P("groups", "mp", None),
            P("groups", "mp", None),
            P("mp", None, "seq"),
            P("mp", "seq", None),
            P("mp", "seq"),
            P("groups", None),
            P("groups"),
        ),
        out_specs=P("groups", ("seq", "mp")),
        check_vma=False,
    )
```

```python
import functools

import jax
import jax.numpy as jnp
from jax import lax
from jax.experimental import pallas as pl
from jax.experimental.pallas import tpu as pltpu
from jax.sharding import PartitionSpec as P

NEG = -1e30
MESH = pl.DeviceIdType.MESH
GROUP = 8
F32 = jnp.float32
BF16 = jnp.bfloat16


def greet(n, me, partner=None):
    barrier = pltpu.get_barrier_semaphore()
    for k in range(1, n):
        peer = lax.rem(me + k, n)
        pl.semaphore_signal(barrier, inc=1, device_id={"seq": peer}, device_id_type=MESH)
    if partner is not None:
        pl.semaphore_signal(barrier, inc=1, device_id={"mp": partner}, device_id_type=MESH)
    pl.semaphore_wait(barrier, n - 1 + (partner is not None))


def push(n, me, src_of, dst, send, recv):
    copies = []
    for k in range(1, n):
        peer = lax.rem(me + k, n)
        copy = pltpu.make_async_remote_copy(
            src_ref=src_of(peer), dst_ref=dst.at[me], send_sem=send.at[k], recv_sem=recv.at[k],
            device_id={"seq": peer}, device_id_type=MESH,
        )
        copy.start()
        copies.append(copy)
    return copies


def make_plan(first_slot, page, most, lengths_ref, table_ref, plan_ref):
    seqs, pages = table_ref.shape
    slots_dev, wide = most
    table = table_ref[...].astype(F32).T
    logical = lax.broadcasted_iota(jnp.int32, (pages, 1), 0)
    slot = lax.broadcasted_iota(jnp.int32, (pages, slots_dev), 1) + first_slot
    slot = slot.astype(F32)
    fill = []
    for b in range(seqs):
        inside = jnp.clip(lengths_ref[b] - page * logical, 0, page)
        hit = table[:, b:b + 1] == slot
        fill.append(jnp.sum(jnp.where(hit, inside, 0), axis=0, keepdims=True))
    eye = (lax.broadcasted_iota(jnp.int32, (slots_dev, slots_dev), 0)
           == lax.broadcasted_iota(jnp.int32, (slots_dev, slots_dev), 1))
    earlier = (lax.broadcasted_iota(jnp.int32, (slots_dev, slots_dev), 1)
               < lax.broadcasted_iota(jnp.int32, (slots_dev, slots_dev), 0))
    at = lax.broadcasted_iota(jnp.int32, (1, wide), 1)
    start = jnp.zeros((1, 1), jnp.int32)
    owner = jnp.zeros((1, wide), jnp.int32)
    target = jnp.full((slots_dev, 1), -1, jnp.int32)
    column = jnp.zeros((slots_dev, 1), jnp.int32)
    for b in range(seqs):
        owned = fill[b] > 0
        count = jnp.sum(owned.astype(jnp.int32), axis=1, keepdims=True)
        place = jnp.sum(jnp.where(earlier & owned, 1, 0), axis=1, keepdims=True)
        mine = jnp.sum(jnp.where(eye, fill[b], 0), axis=1, keepdims=True)
        target = jnp.where(mine > 0, start * GROUP + place, target)
        column = column + mine
        start = start + (count + GROUP - 1) // GROUP
        owner = owner + (at >= start).astype(jnp.int32)
    match = target == lax.broadcasted_iota(jnp.int32, (slots_dev, wide), 1)
    ids = lax.broadcasted_iota(jnp.int32, (slots_dev, wide), 0)
    plan_ref[0:1, :] = jnp.sum(jnp.where(match, ids, 0), axis=0, keepdims=True)
    plan_ref[1:2, :] = jnp.sum(jnp.where(match, column, 0), axis=0, keepdims=True)
    plan_ref[2:3, :] = jnp.minimum(owner, seqs - 1)
    plan_ref[3:4, :] = jnp.broadcast_to(start, (1, wide))
    plan_ref[4:8, :] = jnp.zeros((4, wide), jnp.int32)


def query_kernel(n, pack, page, lengths_ref, table_ref, rope_ref, q_ref, w_ref, out_ref, plan_ref, spread_ref,
                 raw, flat, gath, wide_rope, send, recv, send2, recv2):
    me = lax.axis_index("seq")
    seqs, heads, _ = q_ref.shape
    cols = w_ref.shape[1]
    partner = me + 1 - 2 * lax.rem(me, 2)
    barrier = pltpu.get_barrier_semaphore()
    for peer in [lax.rem(me + 2 * k, n) for k in range(1, n // 2)] + [partner]:
        pl.semaphore_signal(barrier, inc=1, device_id={"seq": peer}, device_id_type=MESH)
    for b in range(seqs):
        flat[b * heads:(b + 1) * heads, :] = q_ref[b].astype(F32)
    for h in range(heads):
        q = flat[pl.ds(h, seqs, stride=heads), :].astype(BF16)
        raw[h * seqs:(h + 1) * seqs, :] = lax.dot_general(
            q, w_ref[h], (((1,), (1,)), ((), ())), preferred_element_type=F32)
    for b in range(0, seqs, pack):
        parts = [raw[pl.ds(b + j, heads, stride=seqs), :] for j in range(pack)]
        row = parts[0] if pack == 1 else jnp.concatenate(parts, axis=1)
        gath[me, b // pack * heads:(b // pack + 1) * heads, :] = row.astype(BF16)
    pl.semaphore_wait(barrier, n // 2)

    def send_to(block, peer, s, r):
        copy = pltpu.make_async_remote_copy(
            src_ref=gath.at[block], dst_ref=gath.at[block], send_sem=s, recv_sem=r,
            device_id={"seq": peer}, device_id_type=MESH)
        copy.start()
        return copy

    across = [send_to(me, partner, send2.at[0], recv2.at[0])]
    line = [send_to(me, lax.rem(me + 2 * k, n), send.at[k], recv.at[k]) for k in range(1, n // 2)]

    slots_dev = rope_ref.shape[0]
    make_plan(me * slots_dev, page, (slots_dev, plan_ref.shape[1]), lengths_ref, table_ref, plan_ref)
    per = page * 128 // rope_ref.shape[1]
    lane = lax.broadcasted_iota(jnp.int32, (slots_dev, 128), 1) // (128 // per)
    for i in range(rope_ref.shape[1] // 128):
        x = rope_ref[:, i * 128:(i + 1) * 128].astype(F32)
        for j in range(per):
            wide_rope[pl.ds(i * per + j, slots_dev, stride=page), :] = jnp.where(lane == j, x, 0.0)

    def narrow(i, _):
        spread_ref[i] = wide_rope[pl.ds(pl.multiple_of(i * page, page), page), :].astype(BF16)
        return 0

    lax.fori_loop(0, slots_dev, narrow, 0, unroll=4)

    for k in range(1, n // 2):
        line[k - 1].wait_recv()
        across.append(send_to(lax.rem(me - 2 * k + n, n), partner, send2.at[k], recv2.at[k]))
    for copy in line:
        copy.wait_send()
    for copy in across:
        copy.wait()
    for s in range(n):
        for b in range(seqs):
            at = b % pack * cols
            out_ref[b, :, s * cols:(s + 1) * cols] = gath[
                s, b // pack * heads:(b // pack + 1) * heads, at:at + cols]


def attend_kernel(scale, pack, plan_ref, q_ref, qr_ref, rope_ref, latent_ref,
                  out_ref, kbuf, acc, top, total, sems):
    seqs, heads, width = q_ref.shape
    page = latent_ref.shape[1]
    tokens = GROUP * page
    n = out_ref.shape[0]
    cols = width // n
    count = plan_ref[3, 0]
    acc[...] = jnp.zeros_like(acc)
    top[...] = jnp.full(top.shape, NEG, F32)
    total[...] = jnp.zeros_like(total)

    def fetch(c, buf):
        return [pltpu.make_async_copy(
            latent_ref.at[plan_ref[0, c * GROUP + g]], kbuf.at[buf, pl.ds(g * page, page)], sems.at[buf, g])
            for g in range(GROUP)]

    for ahead in range(2):
        @pl.when(count > ahead)
        def _():
            for copy in fetch(ahead, ahead):
                copy.start()

    lane = lax.broadcasted_iota(jnp.int32, (1, tokens), 1)

    def step(c, _):
        buf = lax.rem(c, 3)

        @pl.when(c + 2 < count)
        def _():
            for copy in fetch(c + 2, lax.rem(c + 2, 3)):
                copy.start()

        b = plan_ref[2, c]
        rope = jnp.concatenate([rope_ref[plan_ref[0, c * GROUP + g]] for g in range(GROUP)], axis=0)
        limit = jnp.zeros((1, tokens), jnp.int32)
        for g in range(GROUP):
            limit = jnp.where(lane // page == g, plan_ref[1, c * GROUP + g] + g * page, limit)
        nt = (((1,), (1,)), ((), ()))
        score = lax.dot_general(qr_ref[b], rope, nt, preferred_element_type=F32)
        for copy in fetch(c, buf):
            copy.wait()
        keys = kbuf[buf]
        score = (score + lax.dot_general(q_ref[b], keys, nt, preferred_element_type=F32)) * scale
        score = jnp.where(lane < limit, score, NEG)
        old = top[b][:, :1]
        new = jnp.maximum(old, jnp.max(score, axis=1, keepdims=True))
        weight = jnp.exp(score - new)
        carry = jnp.exp(old - new)
        total[b] = total[b] * carry + jnp.sum(weight, axis=1, keepdims=True)
        top[b] = jnp.broadcast_to(new, top.shape[1:])
        acc[b] = acc[b] * carry + jnp.dot(weight.astype(BF16), keys, preferred_element_type=F32)
        return 0

    lax.fori_loop(0, count, step, 0)

    ids = lax.broadcasted_iota(jnp.int32, (heads, 128), 1)
    extra = jnp.zeros((heads, 128), F32)
    for b in range(seqs):
        inv = 1.0 / jnp.maximum(total[b][:, :1], 1e-30)
        whole = acc[b] * inv
        for s in range(n):
            at = b % pack * cols
            out_ref[s, b // pack * heads:(b // pack + 1) * heads, at:at + cols] = whole[
                :, s * cols:(s + 1) * cols].astype(BF16)
        for k, value in enumerate((top[b], total[b])):
            for j in range(3):
                term = value.astype(BF16).astype(F32)
                extra = jnp.where(ids == (k * 3 + j) * seqs + b, term, extra)
                value = value - term
    base = seqs // pack * heads
    lanes = out_ref.shape[2]
    for s in range(n):
        out_ref[s, base:base + heads, :] = extra[:, :lanes].astype(BF16)


def finish_kernel(n, pack, o_ref, v_ref, w_hbm, out_ref, gath, port, pv, part, vals, lhs, w_buf, res,
                  tx, rx, send1, recv1, send2, recv2, send3, recv3, send4, recv4, wsem):
    me = lax.axis_index("seq")
    half = lax.axis_index("mp")
    heads, cols, vdim = v_ref.shape
    seqs = lhs.shape[0]
    hs = heads // n
    load = pltpu.make_async_copy(w_hbm, w_buf, wsem)
    load.start()
    greet(n, me, 1 - half)
    copies = push(n, me, lambda peer: o_ref.at[peer], gath, send1, recv1)
    gath[me] = o_ref[me]
    for copy in copies:
        copy.wait()

    base = seqs // pack * heads
    tops, sums = [], []
    for s in range(n):
        e = gath[s, base:base + heads, :].astype(F32)
        terms = [e[:, k * seqs:(k + 1) * seqs] for k in range(6)]
        tops.append(terms[0] + terms[1] + terms[2])
        sums.append(terms[3] + terms[4] + terms[5])
    best = functools.reduce(jnp.maximum, tops)
    shares = [x * jnp.exp(t - best) for t, x in zip(tops, sums)]
    inv = 1.0 / functools.reduce(jnp.add, shares)
    shares = [x * inv for x in shares]
    lane = lax.broadcasted_iota(jnp.int32, (heads, pack * cols), 1) // cols
    for p in range(seqs // pack):
        total = jnp.zeros((heads, pack * cols), F32)
        for s in range(n):
            share = jnp.broadcast_to(shares[s][:, p * pack:p * pack + 1], total.shape)
            for j in range(1, pack):
                share = jnp.where(lane == j, shares[s][:, p * pack + j:p * pack + j + 1], share)
            total = total + gath[s, p * heads:(p + 1) * heads, :].astype(F32) * share
        for j in range(pack):
            b = p * pack + j
            port[b * heads:(b + 1) * heads, :] = total[:, j * cols:(j + 1) * cols]
    for h in range(heads):
        x = port[pl.ds(h, seqs, stride=heads), :].astype(BF16)
        pv[h // hs, h % hs * seqs:(h % hs + 1) * seqs, :] = jnp.dot(
            x, v_ref[h], preferred_element_type=F32).astype(BF16)
    copies = push(n, me, lambda peer: pv.at[peer], part, send2, recv2)
    part[me] = pv[me]
    for copy in copies:
        copy.wait()
    total = part[0].astype(F32)
    for s in range(1, n):
        total = total + part[s].astype(F32)
    vals[me] = total.astype(BF16)
    copies = push(n, me, lambda peer: vals.at[me], vals, send3, recv3)
    for copy in copies:
        copy.wait()
    for h in range(heads):
        lhs[:, h * vdim:(h + 1) * vdim] = vals[h // hs, h % hs * seqs:(h % hs + 1) * seqs, :]
    load.wait()
    rows = w_buf.shape[0]
    res[...] = jnp.zeros_like(res)
    cut = 1024

    def body(i, _):
        at = pl.ds(pl.multiple_of(i * cut, cut), cut)
        res[...] += jnp.dot(lhs[:, at], w_buf[at, :], preferred_element_type=F32)
        return 0

    lax.fori_loop(0, rows // cut, body, 0)
    wide = res.shape[1] // 2
    low, high = res[:, :wide], res[:, wide:]
    first = half == 0
    tx[...] = jnp.where(first, high, low)
    copy = pltpu.make_async_remote_copy(
        src_ref=tx, dst_ref=rx, send_sem=send4, recv_sem=recv4,
        device_id={"mp": 1 - half}, device_id_type=MESH)
    copy.start()
    copy.wait()
    out_ref[...] = (jnp.where(first, low, high) + rx[...]).astype(BF16)


def local(n, latent_cache, rope_cache, q_nope, q_rope, w_uk, value_up_weight, w_out, page_table, lengths):
    slots_dev, page, width = latent_cache.shape
    seqs, heads, nope = q_nope.shape
    rope_w = q_rope.shape[2]
    cols = w_uk.shape[2]
    vdim = value_up_weight.shape[2]
    scale = (nope + rope_w) ** (-0.5)
    pack = max(1, min(seqs, 128 // cols))
    lanes = pack * cols
    vm = pl.BlockSpec(memory_space=pltpu.VMEM)
    sm = pl.BlockSpec(memory_space=pltpu.SMEM)
    hbm = pl.BlockSpec(memory_space=pl.ANY)
    dma = pltpu.SemaphoreType.DMA
    params = functools.partial(pltpu.CompilerParams, has_side_effects=True)

    most = (slots_dev + seqs * (GROUP - 1)) // GROUP * GROUP
    per = 128 // rope_w
    q_latent, steps, rope = pl.pallas_call(
        functools.partial(query_kernel, n, pack, page),
        out_shape=(
            jax.ShapeDtypeStruct((seqs, heads, width), BF16),
            jax.ShapeDtypeStruct((8, (most + 127) // 128 * 128), jnp.int32),
            jax.ShapeDtypeStruct((slots_dev, page, 128), BF16),
        ),
        in_specs=[sm, vm, vm, vm, vm], out_specs=(vm, vm, vm),
        scratch_shapes=[
            pltpu.VMEM((heads * seqs, cols), F32),
            pltpu.VMEM((heads * seqs, nope), F32),
            pltpu.VMEM((n, seqs // pack * heads, lanes), BF16),
            pltpu.VMEM((slots_dev * page, 128), F32),
            dma((n // 2,)), dma((n // 2,)), dma((n // 2,)), dma((n // 2,)),
        ],
        compiler_params=params(collective_id=1), name="queries",
    )(lengths, page_table, rope_cache, q_nope, w_uk.transpose(0, 2, 1))

    rows = seqs // pack * heads + heads
    mixed = pl.pallas_call(
        functools.partial(attend_kernel, scale, pack),
        out_shape=jax.ShapeDtypeStruct((n, rows, lanes), BF16),
        in_specs=[sm, vm, vm, vm, hbm], out_specs=vm,
        scratch_shapes=[
            pltpu.VMEM((3, GROUP * page, width), BF16),
            pltpu.VMEM((seqs, heads, width), F32),
            pltpu.VMEM((seqs, heads, 128), F32),
            pltpu.VMEM((seqs, heads, 128), F32),
            dma((3, GROUP)),
        ],
        name="attend",
    )(steps, q_latent, jnp.concatenate([q_rope] * per, axis=2), rope, latent_cache)

    wide = w_out.shape[1]
    hs = heads // n
    return pl.pallas_call(
        functools.partial(finish_kernel, n, pack),
        out_shape=jax.ShapeDtypeStruct((seqs, wide // 2), BF16),
        in_specs=[vm, vm, hbm], out_specs=vm,
        scratch_shapes=[
            pltpu.VMEM((n, rows, lanes), BF16),
            pltpu.VMEM((seqs * heads, cols), F32),
            pltpu.VMEM((n, hs * seqs, vdim), BF16),
            pltpu.VMEM((n, hs * seqs, vdim), BF16),
            pltpu.VMEM((n, hs * seqs, vdim), BF16),
            pltpu.VMEM((seqs, heads * vdim), BF16),
            pltpu.VMEM(w_out.shape, BF16),
            pltpu.VMEM((seqs, wide), F32),
            pltpu.VMEM((seqs, wide // 2), F32),
            pltpu.VMEM((seqs, wide // 2), F32),
            dma((n,)), dma((n,)), dma((n,)), dma((n,)), dma((n,)), dma((n,)), dma, dma, dma,
        ],
        compiler_params=params(collective_id=2, vmem_limit_bytes=48 * 1024 * 1024), name="finish",
    )(mixed, value_up_weight, w_out)


def solution(mesh):
    return jax.shard_map(
        functools.partial(local, mesh.shape["seq"]),
        mesh=mesh,
        in_specs=(
            P(("groups", "seq"), None, None),
            P(("groups", "seq"), None),
            P("groups", "mp", None),
            P("groups", "mp", None),
            P("mp", None, "seq"),
            P("mp", "seq", None),
            P("mp", "seq"),
            P("groups", None),
            P("groups"),
        ),
        out_specs=P("groups", ("seq", "mp")),
        check_vma=False,
    )
```

```python
import functools

import jax
import jax.numpy as jnp
from jax import lax
from jax.experimental import pallas as pl
from jax.experimental.pallas import tpu as pltpu
from jax.sharding import PartitionSpec as P

NEG = -1e30
MESH = pl.DeviceIdType.MESH
GROUP = 8
F32 = jnp.float32
BF16 = jnp.bfloat16


def greet(n, me, partner=None):
    barrier = pltpu.get_barrier_semaphore()
    for k in range(1, n):
        peer = lax.rem(me + k, n)
        pl.semaphore_signal(barrier, inc=1, device_id={"seq": peer}, device_id_type=MESH)
    if partner is not None:
        pl.semaphore_signal(barrier, inc=1, device_id={"mp": partner}, device_id_type=MESH)
    pl.semaphore_wait(barrier, n - 1 + (partner is not None))


def push(n, me, src_of, dst, send, recv):
    copies = []
    for k in range(1, n):
        peer = lax.rem(me + k, n)
        copy = pltpu.make_async_remote_copy(
            src_ref=src_of(peer), dst_ref=dst.at[me], send_sem=send.at[k], recv_sem=recv.at[k],
            device_id={"seq": peer}, device_id_type=MESH,
        )
        copy.start()
        copies.append(copy)
    return copies


def make_plan(first_slot, page, most, lengths_ref, table_ref, plan_ref):
    seqs, pages = table_ref.shape
    slots_dev, wide = most
    table = table_ref[...].astype(F32).T
    logical = lax.broadcasted_iota(jnp.int32, (pages, 1), 0)
    slot = lax.broadcasted_iota(jnp.int32, (pages, slots_dev), 1) + first_slot
    slot = slot.astype(F32)
    fill = []
    for b in range(seqs):
        inside = jnp.clip(lengths_ref[b] - page * logical, 0, page)
        hit = table[:, b:b + 1] == slot
        fill.append(jnp.sum(jnp.where(hit, inside, 0), axis=0, keepdims=True))
    eye = (lax.broadcasted_iota(jnp.int32, (slots_dev, slots_dev), 0)
           == lax.broadcasted_iota(jnp.int32, (slots_dev, slots_dev), 1))
    earlier = (lax.broadcasted_iota(jnp.int32, (slots_dev, slots_dev), 1)
               < lax.broadcasted_iota(jnp.int32, (slots_dev, slots_dev), 0))
    at = lax.broadcasted_iota(jnp.int32, (1, wide), 1)
    start = jnp.zeros((1, 1), jnp.int32)
    owner = jnp.zeros((1, wide), jnp.int32)
    target = jnp.full((slots_dev, 1), -1, jnp.int32)
    column = jnp.zeros((slots_dev, 1), jnp.int32)
    for b in range(seqs):
        owned = fill[b] > 0
        count = jnp.sum(owned.astype(jnp.int32), axis=1, keepdims=True)
        place = jnp.sum(jnp.where(earlier & owned, 1, 0), axis=1, keepdims=True)
        mine = jnp.sum(jnp.where(eye, fill[b], 0), axis=1, keepdims=True)
        target = jnp.where(mine > 0, start * GROUP + place, target)
        column = column + mine
        start = start + (count + GROUP - 1) // GROUP
        owner = owner + (at >= start).astype(jnp.int32)
    match = target == lax.broadcasted_iota(jnp.int32, (slots_dev, wide), 1)
    ids = lax.broadcasted_iota(jnp.int32, (slots_dev, wide), 0)
    plan_ref[0:1, :] = jnp.sum(jnp.where(match, ids, 0), axis=0, keepdims=True)
    plan_ref[1:2, :] = jnp.sum(jnp.where(match, column, 0), axis=0, keepdims=True)
    plan_ref[2:3, :] = jnp.minimum(owner, seqs - 1)
    plan_ref[3:4, :] = jnp.broadcast_to(start, (1, wide))
    plan_ref[4:8, :] = jnp.zeros((4, wide), jnp.int32)


def query_kernel(n, pack, page, lengths_ref, table_ref, rope_ref, q_ref, w_ref, out_ref, plan_ref, spread_ref,
                 raw, flat, gath, wide_rope, send, recv, send2, recv2):
    me = lax.axis_index("seq")
    seqs, heads, _ = q_ref.shape
    cols = w_ref.shape[1]
    partner = me + 1 - 2 * lax.rem(me, 2)
    barrier = pltpu.get_barrier_semaphore()
    for peer in [lax.rem(me + 2 * k, n) for k in range(1, n // 2)] + [partner]:
        pl.semaphore_signal(barrier, inc=1, device_id={"seq": peer}, device_id_type=MESH)
    for b in range(seqs):
        flat[b * heads:(b + 1) * heads, :] = q_ref[b].astype(F32)
    for h in range(heads):
        q = flat[pl.ds(h, seqs, stride=heads), :].astype(BF16)
        raw[h * seqs:(h + 1) * seqs, :] = lax.dot_general(
            q, w_ref[h], (((1,), (1,)), ((), ())), preferred_element_type=F32)
    for b in range(0, seqs, pack):
        parts = [raw[pl.ds(b + j, heads, stride=seqs), :] for j in range(pack)]
        row = parts[0] if pack == 1 else jnp.concatenate(parts, axis=1)
        gath[me, b // pack * heads:(b // pack + 1) * heads, :] = row.astype(BF16)
    pl.semaphore_wait(barrier, n // 2)

    def send_to(block, peer, s, r):
        copy = pltpu.make_async_remote_copy(
            src_ref=gath.at[block], dst_ref=gath.at[block], send_sem=s, recv_sem=r,
            device_id={"seq": peer}, device_id_type=MESH)
        copy.start()
        return copy

    across = [send_to(me, partner, send2.at[0], recv2.at[0])]
    line = [send_to(me, lax.rem(me + 2 * k, n), send.at[k], recv.at[k]) for k in range(1, n // 2)]

    slots_dev = rope_ref.shape[0]
    make_plan(me * slots_dev, page, (slots_dev, plan_ref.shape[1]), lengths_ref, table_ref, plan_ref)
    per = page * 128 // rope_ref.shape[1]
    lane = lax.broadcasted_iota(jnp.int32, (slots_dev, 128), 1) // (128 // per)
    for i in range(rope_ref.shape[1] // 128):
        x = rope_ref[:, i * 128:(i + 1) * 128].astype(F32)
        for j in range(per):
            wide_rope[pl.ds(i * per + j, slots_dev, stride=page), :] = jnp.where(lane == j, x, 0.0)

    def narrow(i, _):
        spread_ref[i] = wide_rope[pl.ds(pl.multiple_of(i * page, page), page), :].astype(BF16)
        return 0

    lax.fori_loop(0, slots_dev, narrow, 0, unroll=4)

    for k in range(1, n // 2):
        line[k - 1].wait_recv()
        across.append(send_to(lax.rem(me - 2 * k + n, n), partner, send2.at[k], recv2.at[k]))
    for copy in line:
        copy.wait_send()
    for copy in across:
        copy.wait()
    for s in range(n):
        for b in range(seqs):
            at = b % pack * cols
            out_ref[b, :, s * cols:(s + 1) * cols] = gath[
                s, b // pack * heads:(b // pack + 1) * heads, at:at + cols]


def attend_kernel(scale, pack, plan_ref, q_ref, qr_ref, rope_ref, latent_ref,
                  out_ref, kbuf, acc, top, total, turn, ready, sems):
    seqs, heads, width = q_ref.shape
    page = latent_ref.shape[1]
    tokens = GROUP * page
    n = out_ref.shape[0]
    cols = width // n
    count = plan_ref[3, 0]
    acc[...] = jnp.zeros_like(acc)
    top[...] = jnp.full(top.shape, NEG, F32)
    total[...] = jnp.zeros_like(total)

    def fetch(c, buf):
        return [pltpu.make_async_copy(
            latent_ref.at[plan_ref[0, c * GROUP + g]], kbuf.at[buf, pl.ds(g * page, page)], sems.at[buf, g])
            for g in range(GROUP)]

    for ahead in range(3):
        @pl.when(count > ahead)
        def _():
            for copy in fetch(ahead, ahead):
                copy.start()

    lane = lax.broadcasted_iota(jnp.int32, (1, tokens), 1)

    for b in range(seqs):
        turn[b] = jnp.concatenate([qr_ref[b]] * (128 // qr_ref.shape[2]), axis=1)

    def score_of(c):
        b = plan_ref[2, c]
        rope = jnp.concatenate([rope_ref[plan_ref[0, c * GROUP + g]] for g in range(GROUP)], axis=0)
        limit = jnp.zeros((1, tokens), jnp.int32)
        for g in range(GROUP):
            limit = jnp.where(lane // page == g, plan_ref[1, c * GROUP + g] + g * page, limit)
        nt = (((1,), (1,)), ((), ()))
        score = lax.dot_general(turn[b], rope, nt, preferred_element_type=F32)
        keys = kbuf[lax.rem(c, 4)]
        score = (score + lax.dot_general(q_ref[b], keys, nt, preferred_element_type=F32)) * scale
        return jnp.where(lane < limit, score, NEG)

    @pl.when(count > 0)
    def _():
        for copy in fetch(0, 0):
            copy.wait()
        ready[...] = score_of(0)

    def step(c, _):
        @pl.when(c + 3 < count)
        def _():
            for copy in fetch(c + 3, lax.rem(c + 3, 4)):
                copy.start()

        @pl.when(c + 1 < count)
        def _():
            for copy in fetch(c + 1, lax.rem(c + 1, 4)):
                copy.wait()

        score = ready[...]
        upcoming = score_of(c + 1)
        b = plan_ref[2, c]
        keys = kbuf[lax.rem(c, 4)]
        old = top[b][:, :1]
        new = jnp.maximum(old, jnp.max(score, axis=1, keepdims=True))
        weight = jnp.exp(score - new)
        carry = jnp.exp(old - new)
        product = jnp.dot(weight.astype(BF16), keys, preferred_element_type=F32)
        total[b] = total[b] * carry + jnp.sum(weight, axis=1, keepdims=True)
        top[b] = jnp.broadcast_to(new, top.shape[1:])
        acc[b] = acc[b] * carry + product
        ready[...] = upcoming
        return 0

    lax.fori_loop(0, count, step, 0)

    ids = lax.broadcasted_iota(jnp.int32, (heads, 128), 1)
    extra = jnp.zeros((heads, 128), F32)
    for b in range(seqs):
        inv = 1.0 / jnp.maximum(total[b][:, :1], 1e-30)
        whole = acc[b] * inv
        for s in range(n):
            at = b % pack * cols
            out_ref[s, b // pack * heads:(b // pack + 1) * heads, at:at + cols] = whole[
                :, s * cols:(s + 1) * cols].astype(BF16)
        for k, value in enumerate((top[b], total[b])):
            for j in range(3):
                term = value.astype(BF16).astype(F32)
                extra = jnp.where(ids == (k * 3 + j) * seqs + b, term, extra)
                value = value - term
    base = seqs // pack * heads
    lanes = out_ref.shape[2]
    for s in range(n):
        out_ref[s, base:base + heads, :] = extra[:, :lanes].astype(BF16)


def finish_kernel(n, pack, o_ref, v_ref, w_hbm, out_ref, gath, port, pv, part, vals, lhs, w_buf, res,
                  tx, rx, send1, recv1, send2, recv2, send3, recv3, send4, recv4, wsem):
    me = lax.axis_index("seq")
    half = lax.axis_index("mp")
    heads, cols, vdim = v_ref.shape
    seqs = lhs.shape[0]
    hs = heads // n
    load = pltpu.make_async_copy(w_hbm, w_buf, wsem)
    load.start()
    greet(n, me, 1 - half)
    copies = push(n, me, lambda peer: o_ref.at[peer], gath, send1, recv1)
    gath[me] = o_ref[me]
    for copy in copies:
        copy.wait()

    base = seqs // pack * heads
    tops, sums = [], []
    for s in range(n):
        e = gath[s, base:base + heads, :].astype(F32)
        terms = [e[:, k * seqs:(k + 1) * seqs] for k in range(6)]
        tops.append(terms[0] + terms[1] + terms[2])
        sums.append(terms[3] + terms[4] + terms[5])
    best = functools.reduce(jnp.maximum, tops)
    shares = [x * jnp.exp(t - best) for t, x in zip(tops, sums)]
    inv = 1.0 / functools.reduce(jnp.add, shares)
    shares = [x * inv for x in shares]
    lane = lax.broadcasted_iota(jnp.int32, (heads, pack * cols), 1) // cols
    for p in range(seqs // pack):
        total = jnp.zeros((heads, pack * cols), F32)
        for s in range(n):
            share = jnp.broadcast_to(shares[s][:, p * pack:p * pack + 1], total.shape)
            for j in range(1, pack):
                share = jnp.where(lane == j, shares[s][:, p * pack + j:p * pack + j + 1], share)
            total = total + gath[s, p * heads:(p + 1) * heads, :].astype(F32) * share
        for j in range(pack):
            b = p * pack + j
            port[b * heads:(b + 1) * heads, :] = total[:, j * cols:(j + 1) * cols]
    for h in range(heads):
        x = port[pl.ds(h, seqs, stride=heads), :].astype(BF16)
        pv[h // hs, h % hs * seqs:(h % hs + 1) * seqs, :] = jnp.dot(
            x, v_ref[h], preferred_element_type=F32).astype(BF16)
    copies = push(n, me, lambda peer: pv.at[peer], part, send2, recv2)
    part[me] = pv[me]
    for copy in copies:
        copy.wait()
    total = part[0].astype(F32)
    for s in range(1, n):
        total = total + part[s].astype(F32)
    vals[me] = total.astype(BF16)
    copies = push(n, me, lambda peer: vals.at[me], vals, send3, recv3)
    load.wait()
    rows = hs * vdim
    for k in range(n):
        src = lax.rem(me - k + n, n)
        if k:
            copies[k - 1].wait_recv()
        for h in range(hs):
            lhs[:, h * vdim:(h + 1) * vdim] = vals[src, h * seqs:(h + 1) * seqs, :]
        at = pl.ds(pl.multiple_of(src * rows, rows), rows)
        product = jnp.dot(lhs[...], w_buf[at, :], preferred_element_type=F32)
        if k:
            res[...] += product
        else:
            res[...] = product
    for copy in copies:
        copy.wait_send()
    wide = res.shape[1] // 2
    low, high = res[:, :wide], res[:, wide:]
    first = half == 0
    tx[...] = jnp.where(first, high, low)
    copy = pltpu.make_async_remote_copy(
        src_ref=tx, dst_ref=rx, send_sem=send4, recv_sem=recv4,
        device_id={"mp": 1 - half}, device_id_type=MESH)
    copy.start()
    copy.wait()
    out_ref[...] = (jnp.where(first, low, high) + rx[...]).astype(BF16)


def local(n, latent_cache, rope_cache, q_nope, q_rope, w_uk, value_up_weight, w_out, page_table, lengths):
    slots_dev, page, width = latent_cache.shape
    seqs, heads, nope = q_nope.shape
    rope_w = q_rope.shape[2]
    cols = w_uk.shape[2]
    vdim = value_up_weight.shape[2]
    scale = (nope + rope_w) ** (-0.5)
    pack = max(1, min(seqs, 128 // cols))
    lanes = pack * cols
    vm = pl.BlockSpec(memory_space=pltpu.VMEM)
    sm = pl.BlockSpec(memory_space=pltpu.SMEM)
    hbm = pl.BlockSpec(memory_space=pl.ANY)
    dma = pltpu.SemaphoreType.DMA
    params = functools.partial(pltpu.CompilerParams, has_side_effects=True)

    most = (slots_dev + seqs * (GROUP - 1)) // GROUP * GROUP
    q_latent, steps, rope = pl.pallas_call(
        functools.partial(query_kernel, n, pack, page),
        out_shape=(
            jax.ShapeDtypeStruct((seqs, heads, width), BF16),
            jax.ShapeDtypeStruct((8, (most + GROUP + 127) // 128 * 128), jnp.int32),
            jax.ShapeDtypeStruct((slots_dev, page, 128), BF16),
        ),
        in_specs=[sm, vm, vm, vm, vm], out_specs=(vm, vm, vm),
        scratch_shapes=[
            pltpu.VMEM((heads * seqs, cols), F32),
            pltpu.VMEM((heads * seqs, nope), F32),
            pltpu.VMEM((n, seqs // pack * heads, lanes), BF16),
            pltpu.VMEM((slots_dev * page, 128), F32),
            dma((n // 2,)), dma((n // 2,)), dma((n // 2,)), dma((n // 2,)),
        ],
        compiler_params=params(collective_id=1, vmem_limit_bytes=58 * 1024 * 1024), name="queries",
    )(lengths, page_table, rope_cache, q_nope, w_uk.transpose(0, 2, 1))

    rows = seqs // pack * heads + heads
    mixed = pl.pallas_call(
        functools.partial(attend_kernel, scale, pack),
        out_shape=jax.ShapeDtypeStruct((n, rows, lanes), BF16),
        in_specs=[sm, vm, vm, vm, hbm], out_specs=vm,
        scratch_shapes=[
            pltpu.VMEM((4, GROUP * page, width), BF16),
            pltpu.VMEM((seqs, heads, width), F32),
            pltpu.VMEM((seqs, heads, 128), F32),
            pltpu.VMEM((seqs, heads, 128), F32),
            pltpu.VMEM((seqs, heads, 128), BF16),
            pltpu.VMEM((heads, GROUP * page), F32),
            dma((4, GROUP)),
        ],
        compiler_params=pltpu.CompilerParams(vmem_limit_bytes=58 * 1024 * 1024),
        name="attend",
    )(steps, q_latent, q_rope, rope, latent_cache)

    wide = w_out.shape[1]
    hs = heads // n
    return pl.pallas_call(
        functools.partial(finish_kernel, n, pack),
        out_shape=jax.ShapeDtypeStruct((seqs, wide // 2), BF16),
        in_specs=[vm, vm, hbm], out_specs=vm,
        scratch_shapes=[
            pltpu.VMEM((n, rows, lanes), BF16),
            pltpu.VMEM((seqs * heads, cols), F32),
            pltpu.VMEM((n, hs * seqs, vdim), BF16),
            pltpu.VMEM((n, hs * seqs, vdim), BF16),
            pltpu.VMEM((n, hs * seqs, vdim), BF16),
            pltpu.VMEM((seqs, hs * vdim), BF16),
            pltpu.VMEM(w_out.shape, BF16),
            pltpu.VMEM((seqs, wide), F32),
            pltpu.VMEM((seqs, wide // 2), F32),
            pltpu.VMEM((seqs, wide // 2), F32),
            dma((n,)), dma((n,)), dma((n,)), dma((n,)), dma((n,)), dma((n,)), dma, dma, dma,
        ],
        compiler_params=params(collective_id=2, vmem_limit_bytes=58 * 1024 * 1024), name="finish",
    )(mixed, value_up_weight, w_out)


def solution(mesh):
    return jax.shard_map(
        functools.partial(local, mesh.shape["seq"]),
        mesh=mesh,
        in_specs=(
            P(("groups", "seq"), None, None),
            P(("groups", "seq"), None),
            P("groups", "mp", None),
            P("groups", "mp", None),
            P("mp", None, "seq"),
            P("mp", "seq", None),
            P("mp", "seq"),
            P("groups", None),
            P("groups"),
        ),
        out_specs=P("groups", ("seq", "mp")),
        check_vma=False,
    )
```
